32 devices in a mesh: tp: 2 (over x), cp: 16 (over z, y, core).
Axes of the slice: x: 2, y: 2, z: 4, core: 2. Of those that a mesh axis runs over, the one named last changes fastest.
Arguments:
- query: bfloat16 [6, 2048, 32, 128], P(None, 'cp', 'tp'), parts along dimension 2
- keys: bfloat16 [6, 2048, 8, 128], P(None, 'cp', 'tp'), parts along dimension 2
- values: bfloat16 [6, 2048, 8, 128], P(None, 'cp', 'tp'), parts along dimension 2
- positions: int32 [6, 2048], P(None, 'cp')
- grad_out: bfloat16 [6, 2048, 32, 128], P(None, 'cp', 'tp'), parts along dimension 2
Outputs:
- output 1: bfloat16 [6, 2048, 32, 128], P(None, 'cp', 'tp'), parts along dimension 2
- output 2: bfloat16 [6, 2048, 32, 128], P(None, 'cp', 'tp'), parts along dimension 2
- output 3: bfloat16 [6, 2048, 8, 128], P(None, 'cp', 'tp'), parts along dimension 2
- output 4: bfloat16 [6, 2048, 8, 128], P(None, 'cp', 'tp'), parts along dimension 2
There are 2 independent parts. The reference program is written for one: setup_inputs(seed, part) draws one part's arguments, and reference() takes and returns one part's arrays. A program takes and returns all parts, laid end to end along the dimension named above; an argument that names none is the same for every part.
All inputs are finite; a program needn't handle non-finite values.
Results may differ from the reference program's by a relative error of at most 0.00821769.
Values are sent between devices in bfloat16 or wider.
A program may use at most 1 GiB of HBM per device.

```python
import jax
import jax.numpy as jnp
from jax import lax

BATCH = 6
SEQ_LEN = 2048
CP_SIZE = 16
PART_HEADS = 16
PART_KV_HEADS = 4
HEAD_DIM = 128
ROPE_THETA = 1000000
QUERY_BLOCK = 128

GROUP_SIZE = PART_HEADS // PART_KV_HEADS
LOCAL_LEN = SEQ_LEN // CP_SIZE
HALF_LEN = LOCAL_LEN // 2
NUM_BLOCKS = SEQ_LEN // QUERY_BLOCK


def layout_index():
    stored = jnp.arange(SEQ_LEN, dtype=jnp.int32)
    device = stored // LOCAL_LEN
    within = stored % LOCAL_LEN
    piece_id = jnp.where(within < HALF_LEN, device, 2 * CP_SIZE - 1 - device)
    return piece_id * HALF_LEN + within % HALF_LEN


def draw_positions(pos_key):
    offset_key, gap_key = jax.random.split(pos_key)
    offsets = jax.random.randint(offset_key, (BATCH, 1), 0, SEQ_LEN, dtype=jnp.int32)
    gaps = jax.random.randint(gap_key, (BATCH, SEQ_LEN), 1, 3, dtype=jnp.int32)
    seq_pos = offsets + jnp.cumsum(gaps, axis=1) - gaps[:, :1]
    return jnp.take(seq_pos, layout_index(), axis=1)


def setup_inputs(seed: int = 0, part: int = 0) -> dict:
    base_key = jax.random.key(seed)
    shared_key, part_root = jax.random.split(base_key)
    part_key = jax.random.fold_in(part_root, part)
    key_query, key_keys, key_values, key_grad = jax.random.split(part_key, 4)
    q_shape = (BATCH, SEQ_LEN, PART_HEADS, HEAD_DIM)
    kv_shape = (BATCH, SEQ_LEN, PART_KV_HEADS, HEAD_DIM)
    return {
        'query': jax.random.normal(key_query, q_shape, jnp.float32).astype(jnp.bfloat16),
        'keys': jax.random.normal(key_keys, kv_shape, jnp.float32).astype(jnp.bfloat16),
        'values': jax.random.normal(key_values, kv_shape, jnp.float32).astype(jnp.bfloat16),
        'positions': draw_positions(shared_key),
        'grad_out': jax.random.normal(key_grad, q_shape, jnp.float32).astype(jnp.bfloat16),
    }


def rotary(tensor, positions, angle_sign):
    half_dim = HEAD_DIM // 2
    freq_expo = jnp.arange(half_dim, dtype=jnp.float32) * (2.0 / HEAD_DIM)
    inv_freq = 1.0 / (ROPE_THETA ** freq_expo)
    angles = positions.astype(jnp.float32)[:, :, None] * inv_freq
    cosine = jnp.cos(angles)[:, :, None, :]
    sine_val = angle_sign * jnp.sin(angles)[:, :, None, :]
    pairs = tensor.astype(jnp.float32).reshape(tensor.shape[:-1] + (half_dim, 2))
    even_part = pairs[..., 0]
    odd_part = pairs[..., 1]
    new_even = even_part * cosine - odd_part * sine_val
    new_odd = even_part * sine_val + odd_part * cosine
    return jnp.stack([new_even, new_odd], axis=-1).reshape(tensor.shape)


def reference(query, keys, values, positions, grad_out):
    score_scale = HEAD_DIM ** -0.5
    q_rot = rotary(query, positions, 1.0).astype(jnp.bfloat16)
    k_rot = rotary(keys, positions, 1.0).astype(jnp.bfloat16)

    def by_group(tensor):
        grouped = tensor.reshape(BATCH, NUM_BLOCKS, QUERY_BLOCK, PART_KV_HEADS, GROUP_SIZE, HEAD_DIM)
        grouped = grouped.transpose(0, 3, 1, 2, 4, 5)
        return grouped.reshape(BATCH * PART_KV_HEADS, NUM_BLOCKS, QUERY_BLOCK, GROUP_SIZE, HEAD_DIM)

    def by_kv(tensor):
        return tensor.transpose(0, 2, 1, 3).reshape(BATCH * PART_KV_HEADS, SEQ_LEN, HEAD_DIM)

    pos_rows = jnp.repeat(positions, PART_KV_HEADS, axis=0)

    def one_group(operands):
        q_blocks, k_group, v_group, g_blocks, pos_group = operands
        k_wide = k_group.astype(jnp.float32)
        v_wide = v_group.astype(jnp.float32)
        qpos_blocks = pos_group.reshape(NUM_BLOCKS, QUERY_BLOCK)

        def block_step(acc_pair, blk_inputs):
            dk_acc, dv_acc = acc_pair
            q_blk, g_blk, q_pos = blk_inputs
            q_wide = q_blk.astype(jnp.float32)
            g_wide = g_blk.astype(jnp.float32)
            scores = jnp.einsum('qgd,kd->gqk', q_wide, k_wide) * score_scale
            visible = pos_group[None, :] <= q_pos[:, None]
            scores = jnp.where(visible[None], scores, -jnp.inf)
            weights = jax.nn.softmax(scores, axis=-1)
            out_blk = jnp.einsum('gqk,kd->qgd', weights, v_wide)
            grad_weights = jnp.einsum('qgd,kd->gqk', g_wide, v_wide)
            row_delta = jnp.sum(weights * grad_weights, axis=-1, keepdims=True)
            grad_scores = weights * (grad_weights - row_delta) * score_scale
            dq_blk = jnp.einsum('gqk,kd->qgd', grad_scores, k_wide)
            dk_acc = dk_acc + jnp.einsum('gqk,qgd->kd', grad_scores, q_wide)
            dv_acc = dv_acc + jnp.einsum('gqk,qgd->kd', weights, g_wide)
            return (dk_acc, dv_acc), (out_blk, dq_blk)

        zero_kv = jnp.zeros((SEQ_LEN, HEAD_DIM), jnp.float32)
        sums, per_block = lax.scan(block_step, (zero_kv, zero_kv), (q_blocks, g_blocks, qpos_blocks))
        return per_block[0], per_block[1], sums[0], sums[1]

    out_all, dq_all, dk_all, dv_all = lax.map(
        one_group, (by_group(q_rot), by_kv(k_rot), by_kv(values), by_group(grad_out), pos_rows))

    def from_group(tensor):
        grouped = tensor.reshape(BATCH, PART_KV_HEADS, NUM_BLOCKS, QUERY_BLOCK, GROUP_SIZE, HEAD_DIM)
        return grouped.transpose(0, 2, 3, 1, 4, 5).reshape(BATCH, SEQ_LEN, PART_HEADS, HEAD_DIM)

    def from_kv(tensor):
        return tensor.reshape(BATCH, PART_KV_HEADS, SEQ_LEN, HEAD_DIM).transpose(0, 2, 1, 3)

    attn_out = from_group(out_all).astype(jnp.bfloat16)
    grad_query = rotary(from_group(dq_all), positions, -1.0).astype(jnp.bfloat16)
    grad_keys = rotary(from_kv(dk_all), positions, -1.0).astype(jnp.bfloat16)
    grad_values = from_kv(dv_all).astype(jnp.bfloat16)
    return (attn_out, grad_query, grad_keys, grad_values)
```

```python
import functools

import jax
import jax.numpy as jnp
import numpy as np
from jax import lax
from jax.experimental import pallas as pl
from jax.experimental.pallas import tpu as pltpu
from jax.sharding import PartitionSpec as P

INTERPRET = False
ROPE_THETA = 1000000.0
LOG2E = 1.4426950408889634
ORDER = (0, 2, 4, 6, 7, 5, 3, 1)
RING_POS = tuple(ORDER.index(c) for c in range(8))
NC = 8
STREAMS = 3
BF16, F32 = jnp.bfloat16, jnp.float32


def dg(a, b, ca, cb):
    return lax.dot_general(a, b, (((ca,), (cb,)), ((), ())), preferred_element_type=F32)


def swap_pairs(x):
    lane = lax.broadcasted_iota(jnp.int32, x.shape, x.ndim - 1)
    width = x.shape[-1]
    up = pltpu.roll(x, width - 1, x.ndim - 1)
    down = pltpu.roll(x, 1, x.ndim - 1)
    return jnp.where(lane % 2 == 0, up, down)


def attn_kernel(sel_ref, q_ref, g_ref, cos_ref, sin_ref, *refs):
    kv_refs = refs[:NC - 1]
    ko_ref, vo_ref = refs[NC - 1:NC + 1]
    o_ref, dq_ref, dkv_ref = refs[NC + 1:NC + 4]
    kall, vall, qr, gs, s_a, s_b, m_sc, l_sc, o_t, dq_t, dl_sc = refs[NC + 4:]
    rows = qr.shape[1]
    tok = cos_ref.shape[-2]
    group = rows // tok
    hd = qr.shape[2]
    scale = hd ** -0.5
    core = sel_ref[NC]

    for j in range(NC - 1):
        for lt in range(2):
            kall[lt, j] = kv_refs[j][0, lt]
            vall[lt, j] = kv_refs[j][0, 2 + lt]
    for lt in range(2):
        kall[lt, NC - 1] = ko_ref[0, lt]
        vall[lt, NC - 1] = vo_ref[0, lt]

    for lt in range(2):
        cos = cos_ref[0, lt]
        sin = sin_ref[0, lt]
        for h in range(group):
            x = q_ref[0, lt * group + h].astype(F32)
            qr[lt, h * tok:(h + 1) * tok] = (x * cos + swap_pairs(x) * sin).astype(BF16)
            gs[lt, h * tok:(h + 1) * tok] = g_ref[0, lt * group + h]

    def own_index(shape, dim, lt):
        i = lax.broadcasted_iota(jnp.int32, shape, dim) % tok
        half = tok // 2
        mine_first = (core == 0) if lt == 0 else (core == 1)
        flipped = jnp.where(i < half, i + half, i - half)
        return jnp.where(mine_first, i, flipped)

    neg = -jnp.inf
    for lt in range(2):
        s = dg(kall[lt, 0], qr[lt], 1, 1)
        vis = own_index(s.shape, 0, lt) <= own_index(s.shape, 1, lt)
        s = jnp.where(vis, s, neg)
        s_b[lt] = s
        m_sc[lt] = jnp.max(s, axis=0, keepdims=True)
    for j in range(NC):
        s = dg(kall[0, j], qr[1], 1, 1)
        s_a[j] = s
        m_sc[1] = jnp.maximum(m_sc[1], jnp.max(s, axis=0, keepdims=True))
    for j in range(1, NC):
        sel = sel_ref[j]
        s = dg(kall[sel, j], qr[sel], 1, 1)
        s_b[j + 1] = s
        m_sc[sel] = jnp.maximum(m_sc[sel], jnp.max(s, axis=0, keepdims=True))

    def weights(s, m):
        return jnp.exp2((s - m) * (scale * LOG2E))

    for lt in range(2):
        p = weights(s_b[lt], m_sc[lt])
        s_b[lt] = p
        l_sc[lt] = jnp.sum(p, axis=0, keepdims=True)
        o_t[lt] = dg(vall[lt, 0], p.astype(BF16), 0, 0)
    for j in range(0, NC, 2):
        p = weights(s_a[j:j + 2].reshape(2 * tok, rows), m_sc[1])
        s_a[j:j + 2] = p.reshape(2, tok, rows)
        l_sc[1] += jnp.sum(p, axis=0, keepdims=True)
        o_t[1] += dg(vall[0, j:j + 2].reshape(2 * tok, hd), p.astype(BF16), 0, 0)
    for j in range(1, NC):
        sel = sel_ref[j]
        p = weights(s_b[j + 1], m_sc[sel])
        s_b[j + 1] = p
        l_sc[sel] += jnp.sum(p, axis=0, keepdims=True)
        o_t[sel] += dg(vall[sel, j], p.astype(BF16), 0, 0)

    for lt in range(2):
        inv = 1.0 / l_sc[lt]
        l_sc[lt] = inv
        o = jnp.transpose(o_t[lt] * inv)
        o_ref[0, lt * group:(lt + 1) * group] = o.reshape(group, tok, hd).astype(BF16)
        dl_sc[lt] = jnp.sum(jnp.transpose(o * gs[lt].astype(F32)), axis=0, keepdims=True)

    def grads(p, lt, k, v):
        p = p * l_sc[lt]
        dp = dg(v, gs[lt], 1, 1)
        ds = (p * (dp - dl_sc[lt])).astype(BF16)
        dv = dg(p.astype(BF16), gs[lt], 1, 0)
        dk = dg(ds, qr[lt], 1, 0) * scale
        return dk, dv, dg(k, ds, 0, 0)

    for lt in range(2):
        dk, dv, dq = grads(s_b[lt], lt, kall[lt, 0], vall[lt, 0])
        dkv_ref[0, 0, lt] = dk
        dkv_ref[0, 0, 2 + lt] = dv
        dq_t[lt] = dq
    for j in range(0, NC, 2):
        dk, dv, dq = grads(s_a[j:j + 2].reshape(2 * tok, rows), 1, kall[0, j:j + 2].reshape(2 * tok, hd),
                           vall[0, j:j + 2].reshape(2 * tok, hd))
        dq_t[1] += dq
        for i in range(2):
            if j + i == 0:
                dkv_ref[0, 0, 0] += dk[:tok]
                dkv_ref[0, 0, 2] += dv[:tok]
            else:
                dkv_ref[0, j + i, 0] = dk[i * tok:(i + 1) * tok]
                dkv_ref[0, j + i, 2] = dv[i * tok:(i + 1) * tok]
    for j in range(1, NC):
        sel = sel_ref[j]
        dkv_ref[0, j, 1] = jnp.zeros((tok, hd), F32)
        dkv_ref[0, j, 3] = jnp.zeros((tok, hd), F32)
        dk, dv, dq = grads(s_b[j + 1], sel, kall[sel, j], vall[sel, j])
        dkv_ref[0, j, sel] += dk
        dkv_ref[0, j, 2 + sel] += dv
        dq_t[sel] += dq

    for lt in range(2):
        dq = jnp.transpose(dq_t[lt]) * scale
        cos = cos_ref[0, lt]
        sin = sin_ref[0, lt]
        for h in range(group):
            x = dq[h * tok:(h + 1) * tok]
            dq_ref[0, lt * group + h] = (x * cos - swap_pairs(x) * sin).astype(BF16)


def attention(sel, q, g, cos, sin, chunks, k_opp, v_opp):
    ng, heads2, tok, hd = q.shape
    rows = heads2 // 2 * tok
    nh = ng // cos.shape[0]
    q_spec = pl.BlockSpec((1, heads2, tok, hd), lambda i: (i, 0, 0, 0))
    cs_spec = pl.BlockSpec((1, 2, tok, hd), lambda i: (i // nh, 0, 0, 0))
    kv_spec = pl.BlockSpec((1, 4, tok, hd), lambda i: (i, 0, 0, 0))
    half_spec = pl.BlockSpec((1, 2, tok, hd), lambda i: (i, 0, 0, 0))
    dkv_spec = pl.BlockSpec((1, NC, 4, tok, hd), lambda i: (i, 0, 0, 0, 0))
    flops = ng * 17 * 6 * 2 * tok * rows * hd
    return pl.pallas_call(
        attn_kernel,
        grid=(ng,),
        out_shape=(jax.ShapeDtypeStruct(q.shape, BF16), jax.ShapeDtypeStruct(q.shape, BF16),
                   jax.ShapeDtypeStruct((ng, NC, 4, tok, hd), F32)),
        in_specs=[pl.BlockSpec(memory_space=pltpu.SMEM), q_spec, q_spec, cs_spec, cs_spec]
        + [kv_spec] * (NC - 1) + [half_spec] * 2,
        out_specs=(q_spec, q_spec, dkv_spec),
        scratch_shapes=[
            pltpu.VMEM((2, NC, tok, hd), BF16), pltpu.VMEM((2, NC, tok, hd), BF16),
            pltpu.VMEM((2, rows, hd), BF16), pltpu.VMEM((2, rows, hd), BF16),
            pltpu.VMEM((NC, tok, rows), F32), pltpu.VMEM((NC + 1, tok, rows), F32),
            pltpu.VMEM((2, 1, rows), F32), pltpu.VMEM((2, 1, rows), F32),
            pltpu.VMEM((2, hd, rows), F32), pltpu.VMEM((2, hd, rows), F32),
            pltpu.VMEM((2, 1, rows), F32),
        ],
        compiler_params=pltpu.CompilerParams(dimension_semantics=("arbitrary",),
                                             vmem_limit_bytes=40 * 1024 * 1024),
        cost_estimate=pl.CostEstimate(flops=flops, bytes_accessed=40 * 1024 * 1024, transcendentals=0),
        interpret=INTERPRET,
        name="attn",
    )(sel, q, g, cos, sin, *chunks, k_opp, v_opp)


def rope_kernel(sign, x_ref, cos_ref, sin_ref, o_ref):
    for h in range(x_ref.shape[1]):
        x = x_ref[0, h].astype(F32)
        o_ref[0, h] = (x * cos_ref[0] + (sign * swap_pairs(x)) * sin_ref[0]).astype(BF16)


def rope(x, cos, sin, sign):
    b, h, s, d = x.shape
    x_spec = pl.BlockSpec((1, h, s, d), lambda i: (i, 0, 0, 0))
    c_spec = pl.BlockSpec((1, s, d), lambda i: (i, 0, 0))
    return pl.pallas_call(
        functools.partial(rope_kernel, sign), grid=(b,), out_shape=jax.ShapeDtypeStruct(x.shape, BF16),
        in_specs=[x_spec, c_spec, c_spec], out_specs=x_spec, interpret=INTERPRET, name="rope",
        cost_estimate=pl.CostEstimate(flops=10 * x.size, bytes_accessed=6 * x.size, transcendentals=0))(x, cos, sin)


def tables(positions, head_dim):
    half_dim = head_dim // 2
    freq_expo = jnp.arange(half_dim, dtype=F32) * (2.0 / head_dim)
    inv_freq = 1.0 / (ROPE_THETA ** freq_expo)
    angles = positions.astype(F32)[..., None] * inv_freq
    cosine = jnp.repeat(jnp.cos(angles), 2, axis=-1)
    sine = jnp.repeat(jnp.sin(angles), 2, axis=-1)
    sign = jnp.where(jnp.arange(head_dim) % 2 == 0, -1.0, 1.0).astype(F32)
    return cosine, sine * sign


def solution(mesh):
    cp = mesh.shape['cp']
    nchip = cp // 2
    assert nchip == NC
    pair = [(d, d ^ 1) for d in range(cp)]
    fwd_pairs, bwd_pairs = [], []
    for r in range(NC):
        for core in range(2):
            here = ORDER[r] * 2 + core
            there = ORDER[(r + 1) % NC] * 2 + core
            fwd_pairs.append((here, there))
            bwd_pairs.append((there, here))
    head_spec = P(None, 'cp', 'tp', None)

    def swap(x):
        return lax.ppermute(x, 'cp', pair)

    def up(x):
        return lax.ppermute(x, 'cp', fwd_pairs)

    def down(x):
        return lax.ppermute(x, 'cp', bwd_pairs)

    def local_step(query, keys, values, positions, grad_out):
        nb, length, n_heads, hd = query.shape
        n_kv = keys.shape[2]
        group = n_heads // n_kv
        half = length // 2
        nh = n_kv // 2
        index = lax.axis_index('cp')
        core = index % 2
        chip = index // 2
        ring = jnp.asarray(RING_POS, jnp.int32)[chip]
        order = jnp.asarray(ORDER, jnp.int32)

        cos, sin = tables(positions, hd)
        k_rot = rope(keys.transpose(0, 2, 1, 3), cos, sin, 1.0)
        v_t = values.transpose(0, 2, 1, 3)

        def to_pair(x, axis, size):
            keep = lax.dynamic_slice_in_dim(x, core * size, size, axis)
            send = lax.dynamic_slice_in_dim(x, (1 - core) * size, size, axis)
            return keep, swap(send)

        kv = jnp.stack([k_rot, v_t], axis=2)
        keep, recv = to_pair(kv, 1, nh)
        shape = (nb * nh, 4, half, hd)
        chunk = jnp.stack([keep.reshape(shape), recv.reshape(shape)], axis=2).reshape(nb * nh, 4, length, hd)

        def q_pair(x):
            x = x.transpose(0, 2, 1, 3)
            keep, recv = to_pair(x, 1, nh * group)
            shape = (nb * nh, group, 2, half, hd)
            both = jnp.stack([keep.reshape(shape), recv.reshape(shape)], axis=3)
            return both.transpose(0, 2, 1, 3, 4, 5).reshape(nb * nh, 2 * group, length, hd)

        q_all = q_pair(query)
        g_all = q_pair(grad_out)
        cos2, sin2 = tables(swap(positions), hd)

        def both_tokens(a, b):
            shape = (nb, 2, half, hd)
            return jnp.stack([a.reshape(shape), b.reshape(shape)], axis=2).reshape(nb, 2, length, hd)

        cos_all = both_tokens(cos, cos2)
        sin_all = both_tokens(sin, sin2)

        def later(offset):
            return (order[(ring + offset) % NC] > chip).astype(jnp.int32)

        offsets = [0, -1, 1, -2, 2, -3, 3, 4]
        sel = jnp.stack([later(o) for o in offsets] + [core]).astype(jnp.int32)

        per = nb // STREAMS
        outs, dqs, dks = [], [], []
        for s in range(STREAMS):
            rows = slice(s * per, (s + 1) * per)
            part = slice(s * per * nh, (s + 1) * per * nh)
            own = chunk[part]
            a, b = own, own
            chunks = [own]
            for _ in range(3):
                a, b = up(a), down(b)
                chunks += [a, b]
            k_opp = up(a[:, :2])
            v_opp = down(b[:, 2:])
            out, dq, dkv = attention(sel, q_all[part], g_all[part], cos_all[rows], sin_all[rows],
                                     chunks, k_opp, v_opp)
            to_down = down(dkv[:, 7, :2].astype(BF16)).astype(F32)
            to_up = up(dkv[:, 7, 2:].astype(BF16)).astype(F32)
            to_down = jnp.pad(to_down, ((0, 0), (0, 2), (0, 0), (0, 0)))
            to_up = jnp.pad(to_up, ((0, 0), (2, 0), (0, 0), (0, 0)))
            for h in (2, 1, 0):
                to_down = down((dkv[:, 2 * h + 1] + to_down).astype(BF16)).astype(F32)
                to_up = up((dkv[:, 2 * h + 2] + to_up).astype(BF16)).astype(F32)
            outs.append(out)
            dqs.append(dq)
            dks.append(dkv[:, 0] + to_down + to_up)

        def home(parts):
            x = jnp.concatenate(parts)
            x = x.reshape(nb, nh, 2, group, 2, half, hd)
            def tokens_first(y):
                return y.transpose(0, 2, 4, 1, 3, 5).reshape(nb, length, nh * group, hd)

            keep, recv = tokens_first(x[:, :, :, :, 0]), tokens_first(swap(x[:, :, :, :, 1]))
            return jnp.concatenate([jnp.where(core == 0, keep, recv), jnp.where(core == 0, recv, keep)], axis=2)

        attn_out = home(outs)
        grad_query = home(dqs)

        dkv = jnp.concatenate(dks).reshape(nb, nh, 2, 2 * length, hd)
        dk = rope(dkv[:, :, 0], cos_all.reshape(nb, 2 * length, hd), sin_all.reshape(nb, 2 * length, hd), -1.0)
        dv = dkv[:, :, 1].astype(BF16)
        x = jnp.stack([dk, dv]).reshape(2, nb, nh, 2, 2, half, hd)
        keep, recv = x[:, :, :, :, 0], swap(x[:, :, :, :, 1])
        def tokens_first(y):
            return y.transpose(0, 1, 3, 4, 2, 5).reshape(2, nb, length, nh, hd)

        keep, recv = tokens_first(keep), tokens_first(recv)
        x = jnp.concatenate([jnp.where(core == 0, keep, recv), jnp.where(core == 0, recv, keep)], axis=3)
        return attn_out, grad_query, x[0], x[1]

    return jax.shard_map(local_step, mesh=mesh,
                         in_specs=(head_spec, head_spec, head_spec, P(None, 'cp'), head_spec),
                         out_specs=(head_spec, head_spec, head_spec, head_spec), check_vma=False)
```

```python
import functools

import jax
import jax.numpy as jnp
import numpy as np
from jax import lax
from jax.experimental import pallas as pl
from jax.experimental.pallas import tpu as pltpu
from jax.sharding import PartitionSpec as P

INTERPRET = False
ROPE_THETA = 1000000.0
LOG2E = 1.4426950408889634
ORDER = (0, 2, 4, 6, 7, 5, 3, 1)
RING_POS = tuple(ORDER.index(c) for c in range(8))
NC = 8
STREAMS = 3
BF16, F32 = jnp.bfloat16, jnp.float32


def dg(a, b, ca, cb):
    return lax.dot_general(a, b, (((ca,), (cb,)), ((), ())), preferred_element_type=F32)


def swap_pairs(x):
    lane = lax.broadcasted_iota(jnp.int32, x.shape, x.ndim - 1)
    width = x.shape[-1]
    up = pltpu.roll(x, width - 1, x.ndim - 1)
    down = pltpu.roll(x, 1, x.ndim - 1)
    return jnp.where(lane % 2 == 0, up, down)


def attn_kernel(where, sel_ref, q_ref, g_ref, cos_ref, sin_ref, *refs):
    n_in = max(w[2] for w in where) + 1
    kv_refs = refs[:n_in]
    o_ref, dq_ref, dkv_ref = refs[n_in:n_in + 3]
    kall, vall, qr, gs, s_a, s_b, m_sc, l_sc, o_t, dq_t, dl_sc = refs[n_in + 3:]
    rows = qr.shape[1]
    tok = cos_ref.shape[-2]
    group = rows // tok
    hd = qr.shape[2]
    scale = hd ** -0.5
    core = sel_ref[NC]

    for j, (k, k_at, v, v_at) in enumerate(where):
        for lt in range(2):
            kall[lt, j] = kv_refs[k][0, k_at + lt]
            vall[lt, j] = kv_refs[v][0, v_at + lt]

    for lt in range(2):
        cos = cos_ref[0, lt]
        sin = sin_ref[0, lt]
        for h in range(group):
            x = q_ref[0, lt * group + h].astype(F32)
            qr[lt, h * tok:(h + 1) * tok] = (x * cos + swap_pairs(x) * sin).astype(BF16)
            gs[lt, h * tok:(h + 1) * tok] = g_ref[0, lt * group + h]

    def own_index(shape, dim, lt):
        i = lax.broadcasted_iota(jnp.int32, shape, dim) % tok
        half = tok // 2
        mine_first = (core == 0) if lt == 0 else (core == 1)
        flipped = jnp.where(i < half, i + half, i - half)
        return jnp.where(mine_first, i, flipped)

    neg = -jnp.inf
    for lt in range(2):
        s = dg(kall[lt, 0], qr[lt], 1, 1)
        vis = own_index(s.shape, 0, lt) <= own_index(s.shape, 1, lt)
        s = jnp.where(vis, s, neg)
        s_b[lt] = s
        m_sc[lt] = jnp.max(s, axis=0, keepdims=True)
    for j in range(NC):
        s = dg(kall[0, j], qr[1], 1, 1)
        s_a[j] = s
        m_sc[1] = jnp.maximum(m_sc[1], jnp.max(s, axis=0, keepdims=True))
    for j in range(1, NC):
        sel = sel_ref[j]
        s = dg(kall[sel, j], qr[sel], 1, 1)
        s_b[j + 1] = s
        m_sc[sel] = jnp.maximum(m_sc[sel], jnp.max(s, axis=0, keepdims=True))

    def weights(s, m):
        return jnp.exp2((s - m) * (scale * LOG2E))

    for lt in range(2):
        p = weights(s_b[lt], m_sc[lt])
        s_b[lt] = p
        l_sc[lt] = jnp.sum(p, axis=0, keepdims=True)
        o_t[lt] = dg(vall[lt, 0], p.astype(BF16), 0, 0)
    for j in range(0, NC, 2):
        p = weights(s_a[j:j + 2].reshape(2 * tok, rows), m_sc[1])
        s_a[j:j + 2] = p.reshape(2, tok, rows)
        l_sc[1] += jnp.sum(p, axis=0, keepdims=True)
        o_t[1] += dg(vall[0, j:j + 2].reshape(2 * tok, hd), p.astype(BF16), 0, 0)
    for j in range(1, NC):
        sel = sel_ref[j]
        p = weights(s_b[j + 1], m_sc[sel])
        s_b[j + 1] = p
        l_sc[sel] += jnp.sum(p, axis=0, keepdims=True)
        o_t[sel] += dg(vall[sel, j], p.astype(BF16), 0, 0)

    for lt in range(2):
        inv = 1.0 / l_sc[lt]
        l_sc[lt] = inv
        o = jnp.transpose(o_t[lt] * inv)
        o_ref[0, lt * group:(lt + 1) * group] = o.reshape(group, tok, hd).astype(BF16)
        dl_sc[lt] = jnp.sum(jnp.transpose(o * gs[lt].astype(F32)), axis=0, keepdims=True)

    def grads(p, lt, k, v):
        p = p * l_sc[lt]
        dp = dg(v, gs[lt], 1, 1)
        ds = (p * (dp - dl_sc[lt])).astype(BF16)
        dv = dg(p.astype(BF16), gs[lt], 1, 0)
        dk = dg(ds, qr[lt], 1, 0) * scale
        return dk, dv, dg(k, ds, 0, 0)

    for lt in range(2):
        dk, dv, dq = grads(s_b[lt], lt, kall[lt, 0], vall[lt, 0])
        dkv_ref[0, 0, lt] = dk
        dkv_ref[0, 0, 2 + lt] = dv
        dq_t[lt] = dq
    for j in range(0, NC, 2):
        dk, dv, dq = grads(s_a[j:j + 2].reshape(2 * tok, rows), 1, kall[0, j:j + 2].reshape(2 * tok, hd),
                           vall[0, j:j + 2].reshape(2 * tok, hd))
        dq_t[1] += dq
        for i in range(2):
            if j + i == 0:
                dkv_ref[0, 0, 0] += dk[:tok]
                dkv_ref[0, 0, 2] += dv[:tok]
            else:
                dkv_ref[0, j + i, 0] = dk[i * tok:(i + 1) * tok]
                dkv_ref[0, j + i, 2] = dv[i * tok:(i + 1) * tok]
    for j in range(1, NC):
        sel = sel_ref[j]
        dkv_ref[0, j, 1] = jnp.zeros((tok, hd), F32)
        dkv_ref[0, j, 3] = jnp.zeros((tok, hd), F32)
        dk, dv, dq = grads(s_b[j + 1], sel, kall[sel, j], vall[sel, j])
        dkv_ref[0, j, sel] += dk
        dkv_ref[0, j, 2 + sel] += dv
        dq_t[sel] += dq

    for lt in range(2):
        dq = jnp.transpose(dq_t[lt]) * scale
        cos = cos_ref[0, lt]
        sin = sin_ref[0, lt]
        for h in range(group):
            x = dq[h * tok:(h + 1) * tok]
            dq_ref[0, lt * group + h] = (x * cos - swap_pairs(x) * sin).astype(BF16)


def attention(sel, q, g, cos, sin, first, chunks, ends):
    ng, heads2, tok, hd = q.shape
    rows = heads2 // 2 * tok
    nh = 2
    q_spec = pl.BlockSpec((1, heads2, tok, hd), lambda i: (i, 0, 0, 0))
    cs_spec = pl.BlockSpec((1, 2, tok, hd), lambda i: (first + i // nh, 0, 0, 0))
    kv_spec = pl.BlockSpec((1, 4, tok, hd), lambda i: (i, 0, 0, 0))
    half_spec = pl.BlockSpec((1, 2, tok, hd), lambda i: (i, 0, 0, 0))
    dkv_spec = pl.BlockSpec((1, NC, 4, tok, hd), lambda i: (i, 0, 0, 0, 0))
    flat, where = [], []
    for chunk in list(chunks) + [list(ends)]:
        if isinstance(chunk, list):
            where.append((len(flat), 0, len(flat) + 1, 0))
            flat += chunk
        else:
            where.append((len(flat), 0, len(flat), 2))
            flat.append(chunk)
    specs = [half_spec if x.shape[1] == 2 else kv_spec for x in flat]
    flops = ng * 17 * 6 * 2 * tok * rows * hd
    return pl.pallas_call(
        functools.partial(attn_kernel, tuple(where)),
        grid=(ng,),
        out_shape=(jax.ShapeDtypeStruct(q.shape, BF16), jax.ShapeDtypeStruct(q.shape, BF16),
                   jax.ShapeDtypeStruct((ng, NC, 4, tok, hd), F32)),
        in_specs=[pl.BlockSpec(memory_space=pltpu.SMEM), q_spec, q_spec, cs_spec, cs_spec] + specs,
        out_specs=(q_spec, q_spec, dkv_spec),
        scratch_shapes=[
            pltpu.VMEM((2, NC, tok, hd), BF16), pltpu.VMEM((2, NC, tok, hd), BF16),
            pltpu.VMEM((2, rows, hd), BF16), pltpu.VMEM((2, rows, hd), BF16),
            pltpu.VMEM((NC, tok, rows), F32), pltpu.VMEM((NC + 1, tok, rows), F32),
            pltpu.VMEM((2, 1, rows), F32), pltpu.VMEM((2, 1, rows), F32),
            pltpu.VMEM((2, hd, rows), F32), pltpu.VMEM((2, hd, rows), F32),
            pltpu.VMEM((2, 1, rows), F32),
        ],
        compiler_params=pltpu.CompilerParams(dimension_semantics=("arbitrary",),
                                             vmem_limit_bytes=40 * 1024 * 1024),
        cost_estimate=pl.CostEstimate(flops=flops, bytes_accessed=40 * 1024 * 1024, transcendentals=0),
        interpret=INTERPRET,
        name="attn",
    )(sel, q, g, cos, sin, *flat)


def prep_kernel(k_ref, v_ref, kx_ref, vx_ref, cos_ref, sin_ref, o_ref, wide):
    nh, half = wide.shape[1], wide.shape[0] // 2
    for src, (k, v) in enumerate(((k_ref, v_ref), (kx_ref, vx_ref))):
        to = pl.ds(src * half, half)
        wide[...] = k[0].astype(F32)
        for h in range(nh):
            for lt in range(2):
                x = wide[lt * half:(lt + 1) * half, h]
                o_ref[h, lt, to] = (x * cos_ref[0, lt, to] + swap_pairs(x) * sin_ref[0, lt, to]).astype(BF16)
        wide[...] = v[0].astype(F32)
        for h in range(nh):
            for lt in range(2):
                o_ref[h, 2 + lt, to] = wide[lt * half:(lt + 1) * half, h].astype(BF16)


def prep(k, v, kx, vx, cos, sin, first, count):
    nb, length, nh, hd = k.shape
    x_spec = pl.BlockSpec((1, length, nh, hd), lambda i: (first + i, 0, 0, 0))
    cs_spec = pl.BlockSpec((1, 2, length, hd), lambda i: (first + i, 0, 0, 0))
    return pl.pallas_call(
        prep_kernel, grid=(count,), out_shape=jax.ShapeDtypeStruct((count * nh, 4, length, hd), BF16),
        in_specs=[x_spec] * 4 + [cs_spec] * 2,
        out_specs=pl.BlockSpec((nh, 4, length, hd), lambda i: (i, 0, 0, 0)),
        scratch_shapes=[pltpu.VMEM((length, nh, hd), F32)], interpret=INTERPRET, name="prep",
        cost_estimate=pl.CostEstimate(flops=10 * k.size, bytes_accessed=8 * k.size, transcendentals=0),
    )(k, v, kx, vx, cos, sin)


def final_kernel(dkv_ref, down_ref, up_ref, cos_ref, sin_ref, keep_ref, send_ref):
    half = keep_ref.shape[2]
    for i in range(4):
        x = dkv_ref[0, 0, i] + down_ref[0, i].astype(F32) + up_ref[0, i].astype(F32)
        if i < 2:
            x = x * cos_ref[0, i] - swap_pairs(x) * sin_ref[0, i]
        x = x.astype(BF16)
        keep_ref[0, i] = x[:half]
        send_ref[0, i] = x[half:]


def final(dkv, to_down, to_up, cos, sin, first):
    ng, _, _, tok, hd = dkv.shape
    nh = 2
    half_shape = jax.ShapeDtypeStruct((ng, 4, tok // 2, hd), BF16)
    half_spec = pl.BlockSpec((1, 4, tok // 2, hd), lambda i: (i, 0, 0, 0))
    sum_spec = pl.BlockSpec((1, 4, tok, hd), lambda i: (i, 0, 0, 0))
    cs_spec = pl.BlockSpec((1, 2, tok, hd), lambda i: (first + i // nh, 0, 0, 0))
    return pl.pallas_call(
        final_kernel, grid=(ng,), out_shape=(half_shape, half_shape),
        in_specs=[pl.BlockSpec((1, 1, 4, tok, hd), lambda i: (i, 0, 0, 0, 0)), sum_spec, sum_spec, cs_spec, cs_spec],
        out_specs=(half_spec, half_spec), interpret=INTERPRET, name="final",
        cost_estimate=pl.CostEstimate(flops=ng * 40 * tok * hd, bytes_accessed=ng * 40 * tok * hd, transcendentals=0),
    )(dkv, to_down, to_up, cos, sin)


def after(x, *deps):
    return lax.optimization_barrier((x, *deps))[0]


def tables(positions, head_dim):
    freq_expo = (jnp.arange(head_dim) // 2).astype(F32) * (2.0 / head_dim)
    inv_freq = 1.0 / (ROPE_THETA ** freq_expo)
    angles = positions.astype(F32)[..., None] * inv_freq
    sign = jnp.where(jnp.arange(head_dim) % 2 == 0, -1.0, 1.0).astype(F32)
    return jnp.cos(angles), jnp.sin(angles) * sign


def solution(mesh):
    cp = mesh.shape['cp']
    nchip = cp // 2
    assert nchip == NC
    pair = [(d, d ^ 1) for d in range(cp)]
    fwd_pairs, bwd_pairs = [], []
    for r in range(NC):
        for core in range(2):
            here = ORDER[r] * 2 + core
            there = ORDER[(r + 1) % NC] * 2 + core
            fwd_pairs.append((here, there))
            bwd_pairs.append((there, here))
    head_spec = P(None, 'cp', 'tp', None)

    def swap(x):
        return lax.ppermute(x, 'cp', pair)

    def up(x):
        return lax.ppermute(x, 'cp', fwd_pairs)

    def down(x):
        return lax.ppermute(x, 'cp', bwd_pairs)

    def local_step(query, keys, values, positions, grad_out):
        nb, length, n_heads, hd = query.shape
        n_kv = keys.shape[2]
        group = n_heads // n_kv
        half = length // 2
        nh = n_kv // 2
        index = lax.axis_index('cp')
        core = index % 2
        chip = index // 2
        ring = jnp.asarray(RING_POS, jnp.int32)[chip]
        order = jnp.asarray(ORDER, jnp.int32)

        def cut(x, axis, size, mine):
            return lax.dynamic_slice_in_dim(x, (core if mine else 1 - core) * size, size, axis)

        positions_x = swap(positions)
        k_keep, v_keep = cut(keys, 2, nh, True), cut(values, 2, nh, True)
        k_recv, v_recv = swap(cut(keys, 2, nh, False)), swap(cut(values, 2, nh, False))
        pos_all = jnp.stack([positions.reshape(nb, 2, half), positions_x.reshape(nb, 2, half)], axis=2)
        cos_all, sin_all = tables(pos_all.reshape(nb, 2, length), hd)

        def q_pair(x):
            x = x.transpose(0, 2, 1, 3)
            keep, recv = cut(x, 1, nh * group, True), swap(cut(x, 1, nh * group, False))
            shape = (nb * nh, group, 2, half, hd)
            both = jnp.stack([keep.reshape(shape), recv.reshape(shape)], axis=3)
            return both.transpose(0, 2, 1, 3, 4, 5).reshape(nb * nh, 2 * group, length, hd)

        def later(offset):
            return (order[(ring + offset) % NC] > chip).astype(jnp.int32)

        offsets = [0, -1, 1, -2, 2, -3, 3, 4]
        sel = jnp.stack([later(o) for o in offsets] + [core]).astype(jnp.int32)

        per = nb // STREAMS
        owns = [prep(k_keep, v_keep, k_recv, v_recv, cos_all, sin_all, s * per, per) for s in range(STREAMS)]
        gate = None
        gathered = []
        for s in range(STREAMS):
            own = owns[s]
            if s == 0:
                parts = [own[:, :2], own[:, 2:]]
                chunks = [own]
                a = b = parts
                for _ in range(3):
                    a, b = [up(x) for x in a], [down(x) for x in b]
                    chunks += [a, b]
                gate = chunks[5] + chunks[6]
                ends = [up(a[0]), down(b[1])]
                query, grad_out = after((query, grad_out), chunks[1][0], chunks[2][0])
            else:
                own = after(own, *gate)
                chunks = [own]
                a = b = own
                for _ in range(3):
                    a, b = up(a), down(b)
                    chunks += [a, b]
                gate = chunks[3:5]
                ends = [up(a[:, :2]), down(b[:, 2:])]
            gathered.append((chunks, ends))
        q_all = q_pair(query)
        g_all = q_pair(grad_out)
        outs, dqs, dks = [], [], []
        for s in range(STREAMS):
            part = slice(s * per * nh, (s + 1) * per * nh)
            chunks, ends = gathered[s]
            out, dq, dkv = attention(sel, q_all[part], g_all[part], cos_all, sin_all, s * per, chunks, ends)
            to_down = down(dkv[:, 7, :2].astype(BF16)).astype(F32)
            to_up = up(dkv[:, 7, 2:].astype(BF16)).astype(F32)
            to_down = jnp.pad(to_down, ((0, 0), (0, 2), (0, 0), (0, 0)))
            to_up = jnp.pad(to_up, ((0, 0), (2, 0), (0, 0), (0, 0)))
            for h in (2, 1, 0):
                to_down = down((dkv[:, 2 * h + 1] + to_down.astype(F32)).astype(BF16))
                to_up = up((dkv[:, 2 * h + 2] + to_up.astype(F32)).astype(BF16))
            outs.append(out)
            dqs.append(dq)
            keep, send = final(dkv, to_down, to_up, cos_all, sin_all, s * per)
            dks.append((keep, swap(send)))

        def home(parts):
            x = jnp.concatenate(parts)
            x = x.reshape(nb, nh, 2, group, 2, half, hd)
            def tokens_first(y):
                return y.transpose(0, 2, 4, 1, 3, 5).reshape(nb, length, nh * group, hd)

            keep, recv = tokens_first(x[:, :, :, :, 0]), tokens_first(swap(x[:, :, :, :, 1]))
            return jnp.concatenate([jnp.where(core == 0, keep, recv), jnp.where(core == 0, recv, keep)], axis=2)

        attn_out = home(outs)
        grad_query = home(dqs)

        shape = (nb, nh, 2, 2, half, hd)
        keep = jnp.concatenate([x[0] for x in dks]).reshape(shape).transpose(2, 0, 1, 3, 4, 5)
        recv = jnp.concatenate([x[1] for x in dks]).reshape(shape).transpose(2, 0, 1, 3, 4, 5)

        def tokens_first(y):
            return y.transpose(0, 1, 3, 4, 2, 5).reshape(2, nb, length, nh, hd)

        keep, recv = tokens_first(keep), tokens_first(recv)
        x = jnp.concatenate([jnp.where(core == 0, keep, recv), jnp.where(core == 0, recv, keep)], axis=3)
        return attn_out, grad_query, x[0], x[1]

    return jax.shard_map(local_step, mesh=mesh,
                         in_specs=(head_spec, head_spec, head_spec, P(None, 'cp'), head_spec),
                         out_specs=(head_spec, head_spec, head_spec, head_spec), check_vma=False)
```
